32 devices in a mesh: section: 4 (over z), mp: 8 (over y, x, core).
Axes of the slice: x: 2, y: 2, z: 4, core: 2. Of those that a mesh axis runs over, the one named last changes fastest.
Arguments:
- embeddings: bfloat16 [4, 4, 128, 4096], P('section', None, None, 'mp'), may hold values from -6 to 6
- stored: bfloat16 [4, 3, 128, 4096], P('section', None, None, 'mp'), may hold values from -6 to 6
- dwa_weights: float32 [4, 4], replicated, may hold values from -2.4 to 2.4
- norm_gain: float32 [4, 4096], P('section'), may hold values from 0.5 to 1.5
- qkv_weight: bfloat16 [4, 4096, 3, 4096], P('section', None, None, 'mp')
- out_weight: bfloat16 [4, 4096, 4096], P('section', None, 'mp'), may hold values from -0.09375 to 0.09375
Outputs:
- layer_outputs: bfloat16 [4, 4, 128, 4096], P('section', None, None, 'mp')
The draws below stay inside these ranges and needn't reach their ends.
All inputs are finite; a program needn't handle non-finite values.
Results may differ from the reference program's by a relative error of at most 0.014.
Values may be sent and summed in bfloat16 or wider, within the bound.
A program may use at most 64 MiB of HBM per device.

```python
import jax
import jax.numpy as jnp
from jax import lax

D = 4096
HEADS = 32
HEAD_DIM = 128
TOK = 128
TICKS = 4
SECTIONS = 4
SLOTS = 3


def draw_qkv_weight(key, part):
    base = jax.random.normal(key, (SECTIONS, D, 3, D), jnp.float32) * D ** (-0.5)
    return base.astype(jnp.bfloat16)


def block_levels(own_key, shape, split, low, largest):
    def one(axis_at, shards_of):
        draws = jax.random.uniform(jax.random.fold_in(jax.random.fold_in(own_key, 6), axis_at), (shards_of,), jnp.float32, low / len(split), largest / len(split))
        return jnp.repeat(jnp.exp(draws), shape[axis_at] // shards_of).reshape((-1,) + (1,) * (len(shape) - axis_at - 1))

    gain = one(*split[0])
    for cut in split[1:]:
        gain = gain * one(*cut)
    return gain


def scatter_about(own_key, dims, deviation, limit, cuts=(), held_as=jnp.bfloat16):
    result = deviation * jax.random.normal(own_key, dims, jnp.float32)
    if cuts:
        result = result * block_levels(own_key, dims, cuts, -0.22, 0.18)
    return jnp.clip(result, -limit, limit).astype(held_as)


def setup_inputs(seed: int = 0) -> dict:
    key_list = jax.random.split(jax.random.key(seed), 7)
    return {
        "embeddings": scatter_about(key_list[0], (SECTIONS, TICKS, TOK, D), 1.0, 6.0, ((0, 4), (3, 8))),
        "stored": scatter_about(key_list[1], (SECTIONS, SLOTS, TOK, D), 1.0, 6.0, ((0, 4), (3, 8))),
        "dwa_weights": scatter_about(key_list[2], (SECTIONS, SECTIONS), 0.4, 2.4, (), jnp.float32),
        "norm_gain": jnp.clip(1.0 + 0.1 * jax.random.normal(key_list[3], (SECTIONS, D), jnp.float32), 0.5, 1.5),
        "qkv_weight": draw_qkv_weight(jax.random.fold_in(key_list[6], 71), 0),
        "out_weight": scatter_about(key_list[5], (SECTIONS, D, D), D ** -0.5, 0.09375, ((0, 4), (2, 8))),
    }


EPS = 1e-06

def attend_heads(projected):
    length = projected.shape[0]
    query = projected[:, 0].astype(jnp.float32)
    key_rows = projected[:, 1].astype(jnp.float32)
    value_rows = projected[:, 2].astype(jnp.float32)
    scores = jnp.einsum('qhd,khd->hqk', query, key_rows) * projected.shape[3] ** (-0.5)
    causal = lax.broadcasted_iota(jnp.int32, (length, length), 0) >= lax.broadcasted_iota(jnp.int32, (length, length), 1)
    scores = jnp.where(causal[None], scores, -1e+30)
    row_max = lax.optimization_barrier(jnp.max(scores, axis=2, keepdims=True))
    weights = jnp.exp(scores - row_max)
    probs = (weights / lax.optimization_barrier(jnp.sum(weights, axis=2, keepdims=True))).astype(jnp.bfloat16)
    mixed = jnp.einsum('hqk,khd->qhd', probs.astype(jnp.float32), value_rows)
    return mixed.astype(jnp.bfloat16).reshape(length, -1)

def apply_layer(inputs, gain_row, weight_in, weight_out):
    length = inputs.shape[0]
    values = inputs.astype(jnp.float32)
    inverse = lax.rsqrt(lax.optimization_barrier(jnp.mean(values * values, axis=1, keepdims=True)) + EPS)
    normed = (values * inverse * gain_row).astype(jnp.bfloat16)
    projected = jnp.dot(normed, weight_in.reshape(D, 3 * D), preferred_element_type=jnp.float32).astype(jnp.bfloat16)
    projected = projected.reshape(length, 3, HEADS, HEAD_DIM)
    mixed = attend_heads(projected)
    attn = jnp.dot(mixed, weight_out, preferred_element_type=jnp.float32)
    return (values + attn).astype(jnp.bfloat16)

def reference(embeddings, stored, dwa_weights, norm_gain, qkv_weight, out_weight):
    triangle = jnp.tril(jnp.ones((SECTIONS, SECTIONS), jnp.float32))
    mixing = dwa_weights * triangle
    history = [jnp.concatenate([stored[s], jnp.zeros((TICKS, TOK, D), jnp.bfloat16)], axis=0) for s in range(SECTIONS)]
    results = [[None] * TICKS for s in range(SECTIONS)]
    for step_index in range(TICKS):
        fresh_rows = []
        for section_idx in range(SECTIONS):
            summed = mixing[section_idx, 0] * embeddings[section_idx, step_index].astype(jnp.float32)
            slot_index = step_index - section_idx + SECTIONS - 1
            for source in range(section_idx):
                summed = summed + mixing[section_idx, source + 1] * history[source][slot_index].astype(jnp.float32)
            inputs = summed.astype(jnp.bfloat16)
            fresh_rows.append(apply_layer(inputs, norm_gain[section_idx], qkv_weight[section_idx], out_weight[section_idx]))
        for section_idx in range(SECTIONS):
            slot_index = step_index - section_idx + SECTIONS - 1
            history[section_idx] = history[section_idx].at[slot_index].set(fresh_rows[section_idx])
            results[section_idx][step_index] = fresh_rows[section_idx]
    return jnp.stack([jnp.stack(row_list) for row_list in results])
```

```python
import functools

import jax
import jax.numpy as jnp
from jax import lax
from jax.experimental import pallas as pl
from jax.experimental.pallas import tpu as pltpu
from jax.sharding import PartitionSpec as P

HEAD_DIM = 128
EPS = 1e-06
MESH = pl.DeviceIdType.MESH


def kernel(sections, ranks, groups, mixing, gain, emb_hbm, stored, wqkv_hbm, wout_hbm, out,
           wqkv, wout, emb, rx, xg, hg, summed, acc, acc_out, ssq,
           wqkv_sem, wout_sem, emb_sem, zst_send, zsend, zrecv, xsend, xrecv, hsend, hrecv):
    k = lax.axis_index("section")
    me = lax.axis_index("mp")
    ticks, length, width = emb.shape
    features = width * ranks
    chips = ranks // 2
    chip, core = me // 2, lax.rem(me, 2)
    sib = chip * 2 + 1 - core
    gw = width // groups

    def same(dc):
        return lax.rem(chip + dc, chips) * 2 + core

    def src(dc):
        return lax.rem(chip - dc + chips, chips) * 2 + core

    def sib_src(dc):
        return lax.rem(chip - dc + chips, chips) * 2 + 1 - core

    def rows(blk):
        return pl.ds(pl.multiple_of(blk * width, width), width)

    def load_wqkv(blk):
        return pltpu.make_async_copy(wqkv_hbm.at[:, rows(blk), :], wqkv.at[:, rows(blk), :], wqkv_sem.at[blk])

    emb_copy = pltpu.make_async_copy(emb_hbm, emb, emb_sem)
    wout_copy = pltpu.make_async_copy(wout_hbm, wout, wout_sem)
    emb_copy.start()
    load_wqkv(me).start()
    load_wqkv(sib).start()
    for dc in range(1, chips):
        load_wqkv(src(dc)).start()
    for dc in range(1, chips):
        load_wqkv(sib_src(dc)).start()
    wout_copy.start()

    barrier = pltpu.get_barrier_semaphore()
    for dc in range(1, chips):
        pl.semaphore_signal(barrier, inc=1, device_id=(k, same(dc)), device_id_type=MESH)
    pl.semaphore_signal(barrier, inc=1, device_id=(k, sib), device_id_type=MESH)
    for d in range(1, sections):
        pl.semaphore_signal(barrier, inc=1, device_id=(lax.rem(k + d, sections), me), device_id_type=MESH)
    pl.semaphore_wait(barrier, chips + sections - 1)

    def stored_send(d, t):
        slot = jnp.maximum(t - k - d + sections - 1, 0)
        return pltpu.make_async_remote_copy(
            src_ref=stored.at[slot], dst_ref=rx.at[d - 1, t], send_sem=zst_send.at[d - 1, t],
            recv_sem=zrecv.at[d - 1, t], device_id=(lax.rem(k + d, sections), me), device_id_type=MESH)

    def fresh_send(d, t):
        return pltpu.make_async_remote_copy(
            src_ref=out.at[t], dst_ref=rx.at[d - 1, t + d], send_sem=zsend.at[d - 1, t],
            recv_sem=zrecv.at[d - 1, t + d], device_id=(lax.rem(k + d, sections), me), device_id_type=MESH)

    def fresh_recv(d, t):
        return pltpu.make_async_remote_copy(
            src_ref=out.at[t], dst_ref=rx.at[d - 1, t], send_sem=zsend.at[d - 1, t],
            recv_sem=zrecv.at[d - 1, t], device_id=(lax.rem(k + d, sections), me), device_id_type=MESH)

    for t in range(ticks):
        for d in range(t + 1, sections):
            @pl.when(k + d < sections)
            def _():
                stored_send(d, t).start()

    emb_copy.wait()

    causal = lax.broadcasted_iota(jnp.int32, (length, length), 0) >= lax.broadcasted_iota(
        jnp.int32, (length, length), 1)

    def x_copy(t, blk, send_at, recv_at, target):
        return pltpu.make_async_remote_copy(
            src_ref=xg.at[t, blk], dst_ref=xg.at[t, blk], send_sem=xsend.at[send_at],
            recv_sem=xrecv.at[recv_at], device_id=(k, target), device_id_type=MESH)

    def h_copy(t, g, blk, send_at, recv_at, target):
        return pltpu.make_async_remote_copy(
            src_ref=hg.at[t, g, blk], dst_ref=hg.at[t, g, blk], send_sem=hsend.at[g, send_at],
            recv_sem=hrecv.at[g, recv_at], device_id=(k, target), device_id_type=MESH)

    def tick(t, carry):
        summed[...] = mixing[k, 0] * emb[t].astype(jnp.float32)
        for d in range(sections - 1, 0, -1):
            @pl.when(d <= k)
            def _():
                fresh_recv(d, t).wait_recv()
                summed[...] += mixing[k, jnp.maximum(k - d + 1, 0)] * rx[d - 1, t].astype(jnp.float32)
        xg[t, me] = summed[...].astype(jnp.bfloat16)
        for dc in range(1, chips):
            x_copy(t, me, dc, dc, same(dc)).start()
        x_copy(t, me, chips, chips, sib).start()

        def consume(blk, first=False):
            @pl.when(t == 0)
            def _():
                load_wqkv(blk).wait()
            values = xg[t, blk].astype(jnp.float32)
            part = jnp.sum(values * values, axis=1, keepdims=True)
            scaled = (values * gain[:, rows(blk)]).astype(jnp.bfloat16)
            if first:
                ssq[...] = part
            else:
                ssq[...] += part
            for j in range(3):
                prod = jnp.dot(scaled, wqkv[j, rows(blk), :], preferred_element_type=jnp.float32)
                if first:
                    acc[j] = prod
                else:
                    acc[j] += prod

        consume(me, True)
        x_copy(t, sib, chips, chips, sib).wait_recv()
        consume(sib)

        def direct(dc, c):
            blk = src(dc)
            x_copy(t, blk, dc, dc, sib).wait_recv()
            x_copy(t, blk, chips + dc, chips + dc, sib).start()
            consume(blk)
            return c

        def relayed(dc, c):
            blk = sib_src(dc)
            x_copy(t, blk, chips + dc, chips + dc, sib).wait_recv()
            consume(blk)
            return c

        lax.fori_loop(1, chips, direct, 0)
        lax.fori_loop(1, chips, relayed, 0)

        inverse = lax.rsqrt(ssq[...] * (1.0 / features) + EPS)
        for g in range(groups):
            for h in range(gw // HEAD_DIM):
                cols = pl.ds(g * gw + h * HEAD_DIM, HEAD_DIM)
                q = (acc[0, :, cols] * inverse).astype(jnp.bfloat16)
                kk = (acc[1, :, cols] * inverse).astype(jnp.bfloat16)
                v = (acc[2, :, cols] * inverse).astype(jnp.bfloat16)
                scores = lax.dot_general(q, kk, (((1,), (1,)), ((), ())), preferred_element_type=jnp.float32)
                scores = jnp.where(causal, scores * HEAD_DIM ** -0.5, -1e30)
                weights = jnp.exp(scores - jnp.max(scores, axis=1, keepdims=True))
                probs = (weights / jnp.sum(weights, axis=1, keepdims=True)).astype(jnp.bfloat16)
                mixed = jnp.dot(probs, v, preferred_element_type=jnp.float32).astype(jnp.bfloat16)
                hg[t, g, me, :, pl.ds(h * HEAD_DIM, HEAD_DIM)] = mixed
            for dc in range(1, chips):
                h_copy(t, g, me, dc, dc, same(dc)).start()
            h_copy(t, g, me, chips, chips, sib).start()

        @pl.when(t == 0)
        def _():
            wout_copy.wait()

        def consume_h(g, blk):
            part = pl.ds(pl.multiple_of(blk * width + g * gw, gw), gw)
            acc_out[...] += jnp.dot(hg[t, g, blk], wout[part, :], preferred_element_type=jnp.float32)

        acc_out[...] = xg[t, me].astype(jnp.float32)
        for g in range(groups):
            consume_h(g, me)
        for g in range(groups):
            h_copy(t, g, sib, chips, chips, sib).wait_recv()
            consume_h(g, sib)
        for g in range(groups):
            def h_direct(dc, c):
                blk = src(dc)
                h_copy(t, g, blk, dc, dc, sib).wait_recv()
                h_copy(t, g, blk, chips + dc, chips + dc, sib).start()
                consume_h(g, blk)
                return c

            def h_relayed(dc, c):
                blk = sib_src(dc)
                h_copy(t, g, blk, chips + dc, chips + dc, sib).wait_recv()
                consume_h(g, blk)
                return c

            lax.fori_loop(1, chips, h_direct, 0)
            lax.fori_loop(1, chips, h_relayed, 0)

        out[t] = acc_out[...].astype(jnp.bfloat16)
        for d in range(1, min(sections, ticks)):
            @pl.when((t + d < ticks) & (k + d < sections))
            def _():
                fresh_send(d, t).start()

        def drain(i, c):
            x_copy(t, me, i, i, sib).wait_send()
            for g in range(groups):
                h_copy(t, g, me, i, i, sib).wait_send()
            return c

        lax.fori_loop(1, ranks, drain, 0)
        return carry

    lax.fori_loop(0, ticks, tick, 0)

    for t in range(ticks):
        for d in range(1, sections):
            @pl.when(k + d < sections)
            def _():
                if t < d:
                    stored_send(d, t).wait_send()
                if t + d < ticks:
                    fresh_send(d, t).wait_send()


def local(sections, ranks, embeddings, stored, dwa_weights, norm_gain, qkv_weight, out_weight):
    _, ticks, length, width = embeddings.shape
    features = width * ranks
    heads_here = width // HEAD_DIM
    groups = 2 if heads_here % 2 == 0 else 1
    bf16, f32 = jnp.bfloat16, jnp.float32
    wqkv = jnp.transpose(qkv_weight[0], (1, 0, 2))
    dma = pltpu.SemaphoreType.DMA
    anywhere = pl.BlockSpec(memory_space=pl.ANY)
    result = pl.pallas_call(
        functools.partial(kernel, sections, ranks, groups),
        out_shape=jax.ShapeDtypeStruct((ticks, length, width), bf16),
        in_specs=[pl.BlockSpec(memory_space=pltpu.SMEM), pl.BlockSpec(memory_space=pltpu.VMEM)] + [anywhere] * 4,
        out_specs=pl.BlockSpec(memory_space=pltpu.VMEM),
        scratch_shapes=[
            pltpu.VMEM((3, features, width), bf16),
            pltpu.VMEM((features, width), bf16),
            pltpu.VMEM((ticks, length, width), bf16),
            pltpu.VMEM((sections - 1, ticks, length, width), bf16),
            pltpu.VMEM((ticks, ranks, length, width), bf16),
            pltpu.VMEM((ticks, groups, ranks, length, width // groups), bf16),
            pltpu.VMEM((length, width), f32),
            pltpu.VMEM((3, length, width), f32),
            pltpu.VMEM((length, width), f32),
            pltpu.VMEM((length, 1), f32),
            dma((ranks,)), dma, dma,
            dma((sections - 1, ticks)), dma((sections - 1, ticks)), dma((sections - 1, ticks)),
            dma((ranks,)), dma((ranks,)), dma((groups, ranks)), dma((groups, ranks)),
        ],
        compiler_params=pltpu.CompilerParams(
            collective_id=0, has_side_effects=True, vmem_limit_bytes=60 * 1024 * 1024),
    )(dwa_weights, norm_gain, embeddings[0], stored[0], wqkv, out_weight[0])
    return result[None]


def solution(mesh):
    in_specs = (
        P("section", None, None, "mp"),
        P("section", None, None, "mp"),
        P(),
        P("section", None),
        P("section", None, None, "mp"),
        P("section", None, "mp"),
    )
    out_specs = P("section", None, None, "mp")
    body = functools.partial(local, mesh.shape["section"], mesh.shape["mp"])
    return jax.shard_map(body, mesh=mesh, in_specs=in_specs, out_specs=out_specs, check_vma=False)
```

```python
import functools

import jax
import jax.numpy as jnp
from jax import lax
from jax.experimental import pallas as pl
from jax.experimental.pallas import tpu as pltpu
from jax.sharding import PartitionSpec as P

HEAD_DIM = 128
EPS = 1e-06
PARTS = 2
MESH = pl.DeviceIdType.MESH


def kernel(sections, ranks, parts, mixing, gain, emb_hbm, stored, wqkv_hbm, wout_hbm, out,
           wqkv, wout, emb, rx, xg, hg, summed, acc, proj, acc_out, ssq,
           wqkv_sem, wout_sem, emb_sem, zst_send, zsend, zrecv, xsend, xrecv, hsend, hrecv):
    k = lax.axis_index("section")
    me = lax.axis_index("mp")
    ticks, length, width = emb.shape
    features = width * ranks
    chips = ranks // 2
    chip, core = me // 2, lax.rem(me, 2)
    sib = chip * 2 + 1 - core
    hr = length // parts

    def same(dc):
        return lax.rem(chip + dc, chips) * 2 + core

    def src(dc):
        return lax.rem(chip - dc + chips, chips) * 2 + core

    def sib_src(dc):
        return lax.rem(chip - dc + chips, chips) * 2 + 1 - core

    def rows(blk):
        return pl.ds(pl.multiple_of(blk * width, width), width)

    def load_wqkv(blk):
        return pltpu.make_async_copy(wqkv_hbm.at[:, rows(blk), :], wqkv.at[:, rows(blk), :], wqkv_sem.at[blk])

    emb_copy = pltpu.make_async_copy(emb_hbm, emb, emb_sem)
    wout_copy = pltpu.make_async_copy(wout_hbm, wout, wout_sem)
    emb_copy.start()
    load_wqkv(me).start()
    load_wqkv(sib).start()
    for dc in range(1, chips):
        load_wqkv(src(dc)).start()
    for dc in range(1, chips):
        load_wqkv(sib_src(dc)).start()
    wout_copy.start()

    barrier = pltpu.get_barrier_semaphore()
    for dc in range(1, chips):
        pl.semaphore_signal(barrier, inc=1, device_id=(k, same(dc)), device_id_type=MESH)
    pl.semaphore_signal(barrier, inc=1, device_id=(k, sib), device_id_type=MESH)
    for d in range(1, sections):
        pl.semaphore_signal(barrier, inc=1, device_id=(lax.rem(k + d, sections), me), device_id_type=MESH)
    pl.semaphore_wait(barrier, chips + sections - 1)

    def span(p):
        return pl.ds(p * hr, hr)

    def section_copy(source, at, d, t, p, sems, send_t):
        return pltpu.make_async_remote_copy(
            src_ref=source.at[at, span(p)], dst_ref=rx.at[d - 1, t, span(p)], send_sem=sems.at[d - 1, send_t, p],
            recv_sem=zrecv.at[d - 1, t, p], device_id=(lax.rem(k + d, sections), me), device_id_type=MESH)

    def stored_send(d, t, p):
        return section_copy(stored, jnp.maximum(t - k - d + sections - 1, 0), d, t, p, zst_send, t)

    def fresh_send(d, t, p):
        return section_copy(out, t, d, t + d, p, zsend, t)

    def section_recv(d, t, p):
        return section_copy(out, t, d, t, p, zsend, t)

    def send_stored(low, high):
        for t in range(low, high):
            for p in range(parts):
                for d in range(t + 1, sections):
                    @pl.when(k + d < sections)
                    def _():
                        stored_send(d, t, p).start()

    send_stored(0, 1)

    emb_copy.wait()

    def x_copy(t, p, blk, send_at, recv_at, target):
        return pltpu.make_async_remote_copy(
            src_ref=xg.at[t, blk, span(p)], dst_ref=xg.at[t, blk, span(p)], send_sem=xsend.at[p, send_at],
            recv_sem=xrecv.at[p, recv_at], device_id=(k, target), device_id_type=MESH)

    def h_copy(t, p, blk, send_at, recv_at, target):
        return pltpu.make_async_remote_copy(
            src_ref=hg.at[t, blk, span(p)], dst_ref=hg.at[t, blk, span(p)], send_sem=hsend.at[p, send_at],
            recv_sem=hrecv.at[p, recv_at], device_id=(k, target), device_id_type=MESH)

    def spread(copy, t, p):
        for dc in range(1, chips):
            copy(t, p, me, dc, dc, same(dc)).start()
        copy(t, p, me, chips, chips, sib).start()

    def gather(copy, consume, t, p, early):
        def forward(dc):
            copy(t, p, src(dc), dc, dc, sib).wait_recv()
            copy(t, p, src(dc), chips + dc, chips + dc, sib).start()

        if early:
            for dc in range(1, chips):
                forward(dc)
        consume(me, True)
        copy(t, p, sib, chips, chips, sib).wait_recv()
        consume(sib)

        def direct(dc, c):
            if not early:
                forward(dc)
            consume(src(dc))
            return c

        def relayed(dc, c):
            copy(t, p, sib_src(dc), chips + dc, chips + dc, sib).wait_recv()
            consume(sib_src(dc))
            return c

        lax.fori_loop(1, chips, direct, 0, unroll=chips <= 4)
        lax.fori_loop(1, chips, relayed, 0, unroll=chips <= 4)

    def tick(t, carry):
        for p in range(parts):
            at = span(p)
            summed[at] = mixing[k, 0] * emb[t, at].astype(jnp.float32)
            for d in range(sections - 1, 0, -1):
                @pl.when(d <= k)
                def _():
                    section_recv(d, t, p).wait_recv()
                    summed[at] += mixing[k, jnp.maximum(k - d + 1, 0)] * rx[d - 1, t, at].astype(jnp.float32)
            xg[t, me, at] = summed[at].astype(jnp.bfloat16)
            spread(x_copy, t, p)

        @pl.when(t == 0)
        def _():
            send_stored(1, ticks)

        for p in range(parts):
            at = span(p)

            def consume(blk, first=False):
                if p == 0:
                    @pl.when(t == 0)
                    def _():
                        load_wqkv(blk).wait()
                values = xg[t, blk, at].astype(jnp.float32)
                part = jnp.sum(values * values, axis=1, keepdims=True)
                scaled = (values * gain[:, rows(blk)]).astype(jnp.bfloat16)
                if first:
                    ssq[at] = part
                else:
                    ssq[at] += part
                for j in range(3):
                    prod = jnp.dot(scaled, wqkv[j, rows(blk), :], preferred_element_type=jnp.float32)
                    if first:
                        acc[j, at] = prod
                    else:
                        acc[j, at] += prod

            gather(x_copy, consume, t, p, p > 0)

            inverse = lax.rsqrt(ssq[at] * (1.0 / features) + EPS)
            seen = (p + 1) * hr
            causal = p * hr + lax.broadcasted_iota(jnp.int32, (hr, seen), 0) >= lax.broadcasted_iota(
                jnp.int32, (hr, seen), 1)
            for j in range(3):
                proj[j, at] = (acc[j, at] * inverse).astype(jnp.bfloat16)
            for h in range(width // HEAD_DIM):
                cols = pl.ds(h * HEAD_DIM, HEAD_DIM)
                scores = lax.dot_general(proj[0, at, cols], proj[1, pl.ds(0, seen), cols], (((1,), (1,)), ((), ())),
                                         preferred_element_type=jnp.float32)
                scores = jnp.where(causal, scores * HEAD_DIM ** -0.5, -1e30)
                weights = jnp.exp(scores - jnp.max(scores, axis=1, keepdims=True))
                probs = (weights / jnp.sum(weights, axis=1, keepdims=True)).astype(jnp.bfloat16)
                mixed = jnp.dot(probs, proj[2, pl.ds(0, seen), cols], preferred_element_type=jnp.float32)
                hg[t, me, at, cols] = mixed.astype(jnp.bfloat16)
            spread(h_copy, t, p)

        @pl.when(t == 0)
        def _():
            wout_copy.wait()

        for p in range(parts):
            at = span(p)

            def consume_h(blk, first=False):
                prod = jnp.dot(hg[t, blk, at], wout[rows(blk), :], preferred_element_type=jnp.float32)
                if first:
                    acc_out[at] = xg[t, me, at].astype(jnp.float32) + prod
                else:
                    acc_out[at] += prod

            gather(h_copy, consume_h, t, p, p > 0)
            out[t, at] = acc_out[at].astype(jnp.bfloat16)
            for d in range(1, min(sections, ticks)):
                @pl.when((t + d < ticks) & (k + d < sections))
                def _():
                    fresh_send(d, t, p).start()

        def drain(i, c):
            for p in range(parts):
                x_copy(t, p, me, i, i, sib).wait_send()
                h_copy(t, p, me, i, i, sib).wait_send()
            return c

        lax.fori_loop(1, ranks, drain, 0)
        return carry

    lax.fori_loop(0, ticks, tick, 0)

    for t in range(ticks):
        for d in range(1, sections):
            @pl.when(k + d < sections)
            def _():
                for p in range(parts):
                    if t < d:
                        stored_send(d, t, p).wait_send()
                    if t + d < ticks:
                        fresh_send(d, t, p).wait_send()


def local(sections, ranks, embeddings, stored, dwa_weights, norm_gain, qkv_weight, out_weight):
    _, ticks, length, width = embeddings.shape
    features = width * ranks
    parts = PARTS
    bf16, f32 = jnp.bfloat16, jnp.float32
    wqkv = jnp.transpose(qkv_weight[0], (1, 0, 2))
    dma = pltpu.SemaphoreType.DMA
    anywhere = pl.BlockSpec(memory_space=pl.ANY)
    result = pl.pallas_call(
        functools.partial(kernel, sections, ranks, parts),
        out_shape=jax.ShapeDtypeStruct((ticks, length, width), bf16),
        in_specs=[pl.BlockSpec(memory_space=pltpu.SMEM), pl.BlockSpec(memory_space=pltpu.VMEM)] + [anywhere] * 4,
        out_specs=pl.BlockSpec(memory_space=pltpu.VMEM),
        scratch_shapes=[
            pltpu.VMEM((3, features, width), bf16),
            pltpu.VMEM((features, width), bf16),
            pltpu.VMEM((ticks, length, width), bf16),
            pltpu.VMEM((sections - 1, ticks, length, width), bf16),
            pltpu.VMEM((ticks, ranks, length, width), bf16),
            pltpu.VMEM((ticks, ranks, length, width), bf16),
            pltpu.VMEM((length, width), f32),
            pltpu.VMEM((3, length, width), f32),
            pltpu.VMEM((3, length, width), bf16),
            pltpu.VMEM((length, width), f32),
            pltpu.VMEM((length, 1), f32),
            dma((ranks,)), dma, dma,
            dma((sections - 1, ticks, parts)), dma((sections - 1, ticks, parts)), dma((sections - 1, ticks, parts)),
            dma((parts, ranks)), dma((parts, ranks)), dma((parts, ranks)), dma((parts, ranks)),
        ],
        compiler_params=pltpu.CompilerParams(
            collective_id=0, has_side_effects=True, vmem_limit_bytes=60 * 1024 * 1024),
    )(dwa_weights, norm_gain, embeddings[0], stored[0], wqkv, out_weight[0])
    return result[None]


def solution(mesh):
    in_specs = (
        P("section", None, None, "mp"),
        P("section", None, None, "mp"),
        P(),
        P("section", None),
        P("section", None, None, "mp"),
        P("section", None, "mp"),
    )
    out_specs = P("section", None, None, "mp")
    body = functools.partial(local, mesh.shape["section"], mesh.shape["mp"])
    return jax.shard_map(body, mesh=mesh, in_specs=in_specs, out_specs=out_specs, check_vma=False)
```
